32 devices in a mesh: band: 8 (over z, y), ga: 4 (over x, core).
Axes of the slice: x: 2, y: 2, z: 4, core: 2. Of those that a mesh axis runs over, the one named last changes fastest.
Arguments:
- orbitals: float32 [8, 96, 9216], P('band', 'ga'), may hold values from -6 to 6
- retained: int32 [96, 9216], P(None, 'ga'), may hold values 0 or 1
Outputs:
- exchange_field: float32 [8, 96, 9216], P('band', 'ga')
- block_matrix: float32 [8, 1], P('band')
The draws below stay inside these ranges and needn't reach their ends.
All inputs are finite; a program needn't handle non-finite values. No bound on the sum of `retained` on one device may be relied on, other than what follows from the above.
Results may differ from the reference program's by a relative error of at most 0.0086.
Values may be sent and summed in bfloat16 or wider, within the bound.
No kernel may reach another device: no remote copies, remote signals or barrier semaphores. Data moves between devices by JAX's collectives and lax.ppermute only.
A program may use at most 64 MiB of HBM per device.

```python
import jax
import jax.numpy as jnp
from jax import lax

N = 96
BD = 1
BANDS = 8
REACH = 1
N_BAND = 8


def place_ends(values, key, least, top_value):
    place = [jax.random.randint(jax.random.fold_in(key, axis), (), 0, length) for axis, length in enumerate(values.shape)]
    widest = values.shape.index(max(values.shape))
    beside = place[:widest] + [(place[widest] + 1) % values.shape[widest]] + place[widest + 1:]
    return values.at[tuple(place)].set(least).at[tuple(beside)].set(top_value)


def shard_levels(stream_key, extent, split, least, top_value):
    loudness = 1.0
    for dim, shards_of in split:
        steps = jax.random.uniform(jax.random.fold_in(jax.random.fold_in(stream_key, 6), dim), (shards_of,), jnp.float32, least / len(split), top_value / len(split))
        loudness = loudness * jnp.repeat(jnp.exp(steps), extent[dim] // shards_of).reshape((-1,) + (1,) * (len(extent) - 1 - dim))
    return loudness


def noise(key, extent, deviation, bound, split=(), kind=jnp.bfloat16):
    result = jax.random.normal(key, extent, jnp.float32) * deviation
    if len(split) > 0:
        result = shard_levels(key, extent, split, -0.22, 0.18) * result
    return jnp.clip(result, min=-bound, max=bound).astype(kind)


def setup_inputs(seed: int = 0) -> dict:
    key_list = jax.random.split(jax.random.key(seed), 3)
    return {
        "orbitals": noise(key_list[0], (BANDS, N, N * N), 1.0, 6.0, ((0, 8), (1, 4)), jnp.float32),
        "retained": place_ends((jax.random.randint(key_list[1], (N, N * N), 0, 4) < 3).astype(jnp.int32), jax.random.fold_in(key_list[1], 1), 0, 1),
    }


def cas_table(length):
    counter = jnp.arange(length, dtype=jnp.int32)
    product = counter[:, None] * counter[None, :] % length
    angles = 2.0 * jnp.pi / length * product.astype(jnp.float32)
    scaled = (jnp.cos(angles) + jnp.sin(angles)) / jnp.sqrt(jnp.float32(length))
    return scaled.astype(jnp.bfloat16)

def wrapped(indices, length):
    return jnp.where(indices < length // 2, indices, indices - length).astype(jnp.float32)

def screening(rows_x, rows_y, rows_z, length):
    freq_x = wrapped(rows_x, length)
    freq_y = wrapped(rows_y, length)
    freq_z = wrapped(rows_z, length)
    squared = freq_x[:, None, None] ** 2 + freq_y[None, :, None] ** 2 + freq_z[None, None, :] ** 2
    spread = length / 4.0
    return 1.0 / (1.0 + squared / (spread * spread))

def transform_axis(density, table, form):
    return jnp.einsum(form, density.astype(jnp.float32), table.astype(jnp.float32)).astype(jnp.bfloat16)

def potential(density, table, screen):
    sectioned = transform_axis(density, table, 'pxyz,kz->pxyk')
    sectioned = transform_axis(sectioned, table, 'pxyz,ky->pxkz')
    sectioned = transform_axis(sectioned, table, 'pxyz,kx->pkyz')
    sectioned = (sectioned.astype(jnp.float32) * screen).astype(jnp.bfloat16)
    sectioned = transform_axis(sectioned, table, 'pxyz,kx->pkyz')
    sectioned = transform_axis(sectioned, table, 'pxyz,ky->pxkz')
    return transform_axis(sectioned, table, 'pxyz,kz->pxyk')

def reference(orbitals, retained):
    lattice = orbitals.reshape(BANDS, N, N, N).astype(jnp.float32)
    table = cas_table(N)
    counter = jnp.arange(N, dtype=jnp.int32)
    screen = screening(counter, counter, counter, N) * retained.reshape(N, N, N).astype(jnp.float32)
    window = (2 * REACH + 1) * BD

    def one_block(block):
        offsets = jnp.arange(-REACH * BD, (REACH + 1) * BD, dtype=jnp.int32)
        indices = ((block * BD + offsets) % BANDS).astype(jnp.int32)
        visitors = lattice[indices]
        owned = lax.dynamic_slice_in_dim(lattice, (block * BD).astype(jnp.int32), BD, 0)
        density = (owned[:, None] * visitors[None]).astype(jnp.bfloat16).reshape(BD * window, N, N, N)
        fields = potential(density, table, screen).astype(jnp.float32).reshape(BD, window, N, N, N)
        running = lax.optimization_barrier(jnp.sum(fields * visitors[None], axis=1))
        intersection = jnp.dot(owned.reshape(BD, -1), running.reshape(BD, -1).T, precision=lax.Precision.HIGHEST) / float(N ** 3)
        return (running, intersection)
    fields_all, blocks_all = lax.map(one_block, jnp.arange(N_BAND, dtype=jnp.int32))
    return (fields_all.reshape(BANDS, N, N * N), blocks_all.reshape(BANDS, BD))
```

```python
import math
from functools import partial

import jax
import jax.numpy as jnp
import numpy as np
from jax import lax
from jax.experimental import pallas as pl
from jax.experimental.pallas import tpu as pltpu
from jax.sharding import PartitionSpec as P

LANES = 128


def passed_along(value, axis, steps):
    count = lax.axis_size(axis)
    pairs = [(source, (source + steps) % count) for source in range(count)]
    return lax.ppermute(value, axis, pairs)


def cas_table(length):
    counter = np.arange(length)
    angles = 2.0 * np.pi / length * (counter[:, None] * counter[None, :] % length)
    scaled = (np.cos(angles) + np.sin(angles)) / np.sqrt(float(length))
    return scaled.astype(np.float32).astype(jnp.bfloat16).astype(np.float32)


def wrapped(indices, length):
    return jnp.where(indices < length // 2, indices, indices - length).astype(jnp.float32)


def screening(rows_x, rows_y, rows_z, length):
    freq_x = wrapped(rows_x, length)
    freq_y = wrapped(rows_y, length)
    freq_z = wrapped(rows_z, length)
    squared = freq_x[:, None, None] ** 2 + freq_y[None, :, None] ** 2 + freq_z[None, None, :] ** 2
    spread = length / 4.0
    return 1.0 / (1.0 + squared / (spread * spread))


def lane_of(shape):
    return lax.broadcasted_iota(jnp.int32, shape, len(shape) - 1)


def dense(parts, length):
    spill = LANES - length
    lane = lane_of(parts[0].shape)
    last = parts[-1]
    return [
        jnp.where(lane < length, part, pltpu.roll(last, (length - spill * j) % LANES, last.ndim - 1))
        for j, part in enumerate(parts[:-1])
    ]


def undense(parts, length):
    spill = LANES - length
    lane = lane_of(parts[0].shape)
    last = jnp.zeros_like(parts[0])
    for j, part in enumerate(parts):
        moved = pltpu.roll(part, (spill * j - length) % LANES, part.ndim - 1)
        last = jnp.where((lane >= spill * j) & (lane < spill * (j + 1)), moved, last)
    return last


def dot(a, b):
    return jnp.dot(a, b, preferred_element_type=jnp.float32)


class Sizes:
    def __init__(self, length, rows, groups):
        self.length = length
        self.rows = rows
        self.groups = groups
        self.cols = length // groups
        whole = math.lcm(length, LANES)
        self.pack = whole // length
        self.chunks = whole // LANES
        self.quads = length // self.pack
        self.width = self.pack * length
        self.inner = rows // self.pack
        assert self.chunks == self.pack - 1 and self.inner % 2 == 0 and self.cols % 2 == 0
        self.sent = (groups, self.chunks, self.inner * self.cols, LANES)


def tables(sz):
    table = cas_table(sz.length)
    spread = np.zeros((sz.width, sz.pack * LANES), np.float32)
    for r in range(sz.pack):
        spread[r * sz.length:(r + 1) * sz.length, r * LANES:r * LANES + sz.length] = table
    y_order = np.arange(sz.length).reshape(sz.quads, sz.pack).T.reshape(-1)
    x_all = np.arange(sz.length).reshape(sz.groups, sz.pack, sz.inner)
    x_order = x_all.transpose(1, 0, 2).reshape(-1)
    half = jnp.bfloat16
    return dict(
        z=jnp.asarray(spread, half), zb=jnp.asarray(spread.T, half),
        y=jnp.asarray(table[:, y_order], half), yb=jnp.asarray(table[y_order, :], half),
        x=jnp.asarray(table[:, x_order], half), xb=jnp.asarray(table[x_order, :], half),
    )


def forward_kernel(sz, a_ref, b_ref, z_ref, y_ref, out_ref, s_ref):
    w = sz.width
    rows = jnp.concatenate(
        [
            a_ref[:, q * w:(q + 1) * w] * b_ref[:, q * w:(q + 1) * w].astype(jnp.float32)
            for q in range(sz.quads)
        ],
        axis=0,
    ).astype(jnp.bfloat16)
    spread = dot(rows, z_ref[...])
    for r in range(sz.pack):
        s_ref[r] = spread[:, r * LANES:(r + 1) * LANES]
    for xi in range(0, sz.inner, 2):
        planes = []
        for g in range(sz.pack):
            col = jnp.concatenate(
                [
                    jnp.concatenate(
                        [
                            s_ref[r, pl.ds(g * sz.inner + xi + h, sz.quads, stride=sz.rows), :]
                            for r in range(sz.pack)
                        ],
                        axis=0,
                    )
                    for h in range(2)
                ],
                axis=1,
            ).astype(jnp.bfloat16)
            planes.append(dot(y_ref[...], col))
        packed = [
            dense([plane[:, h * LANES:(h + 1) * LANES] for plane in planes], sz.length)
            for h in range(2)
        ]
        for j in range(sz.chunks):
            for p in range(sz.groups):
                cut = slice(p * sz.cols, (p + 1) * sz.cols)
                out_ref[p, j, xi * sz.cols:(xi + 2) * sz.cols, :] = jnp.concatenate(
                    [packed[0][j][cut], packed[1][j][cut]], axis=0
                ).astype(jnp.bfloat16)


def middle_kernel(sz, r_ref, x_ref, xb_ref, screen_ref, out_ref, sum_ref, f_ref, g_ref):
    span = sz.inner * sz.cols
    for s in range(sz.groups):
        parts = [r_ref[s, j].astype(jnp.float32) for j in range(sz.chunks)]
        for g, part in enumerate(parts + [undense(parts, sz.length)]):
            f_ref[g, s * span:(s + 1) * span, :] = part
    many = sz.groups * sz.inner
    total = jnp.zeros((sz.length, LANES), jnp.float32)
    for ky in range(0, sz.cols, 2):
        col = jnp.concatenate(
            [
                jnp.concatenate(
                    [f_ref[g, pl.ds(ky + h, many, stride=sz.cols), :] for g in range(sz.pack)],
                    axis=0,
                )
                for h in range(2)
            ],
            axis=1,
        ).astype(jnp.bfloat16)
        spectrum = dot(x_ref[...], col).astype(jnp.bfloat16).astype(jnp.float32)
        screen = jnp.concatenate([screen_ref[ky], screen_ref[ky + 1]], axis=1)
        weighted = spectrum * screen
        energy = spectrum * weighted
        total = total + energy[:, :LANES] + energy[:, LANES:]
        back = dot(xb_ref[...], weighted.astype(jnp.bfloat16))
        for h in range(2):
            for g in range(sz.pack):
                g_ref[g, pl.ds(ky + h, many, stride=sz.cols), :] = back[
                    g * many:(g + 1) * many, h * LANES:(h + 1) * LANES
                ]
    sum_ref[...] = jnp.sum(total, axis=0, keepdims=True)
    for s in range(sz.groups):
        parts = [g_ref[g, s * span:(s + 1) * span, :] for g in range(sz.pack)]
        for j, part in enumerate(dense(parts, sz.length)):
            out_ref[s, j] = part.astype(jnp.bfloat16)


def backward_body(sz, r_ref, yb_ref, zb_ref, s_ref):
    for xi in range(0, sz.inner, 2):
        cut = slice(xi * sz.cols, (xi + 2) * sz.cols)
        blocks = []
        for p in range(sz.groups):
            parts = [r_ref[p, j, cut, :].astype(jnp.float32) for j in range(sz.chunks)]
            blocks.append(parts + [undense(parts, sz.length)])
        for g in range(sz.pack):
            col = jnp.concatenate(
                [
                    jnp.concatenate(
                        [blocks[p][g][h * sz.cols:(h + 1) * sz.cols] for p in range(sz.groups)],
                        axis=0,
                    )
                    for h in range(2)
                ],
                axis=1,
            ).astype(jnp.bfloat16)
            plane = dot(yb_ref[...], col)
            for h in range(2):
                for r in range(sz.pack):
                    s_ref[r, pl.ds(g * sz.inner + xi + h, sz.quads, stride=sz.rows), :] = plane[
                        r * sz.quads:(r + 1) * sz.quads, h * LANES:(h + 1) * LANES
                    ]
    rows = jnp.concatenate(
        [s_ref[r].astype(jnp.bfloat16) for r in range(sz.pack)], axis=1
    )
    return dot(rows, zb_ref[...]).astype(jnp.bfloat16).astype(jnp.float32)


def own_kernel(sz, r_ref, a_ref, yb_ref, zb_ref, out_ref, s_ref):
    v = backward_body(sz, r_ref, yb_ref, zb_ref, s_ref)
    for q in range(sz.quads):
        cut = slice(q * sz.width, (q + 1) * sz.width)
        out_ref[:, cut] = v[q * sz.rows:(q + 1) * sz.rows] * a_ref[:, cut]


def cross_kernel(sz, r_ref, a_ref, b_ref, run_ref, yb_ref, zb_ref, out_ref, back_ref, s_ref):
    v = backward_body(sz, r_ref, yb_ref, zb_ref, s_ref)
    for q in range(sz.quads):
        cut = slice(q * sz.width, (q + 1) * sz.width)
        part = v[q * sz.rows:(q + 1) * sz.rows]
        out_ref[:, cut] = run_ref[:, cut] + part * b_ref[:, cut].astype(jnp.float32)
        back_ref[:, cut] = (part * a_ref[:, cut]).astype(back_ref.dtype)


def local(orbitals, retained):
    bands_dev, slab_rows, plane_cells = orbitals.shape
    assert bands_dev == 1
    length = retained.shape[0]
    groups = lax.axis_size("ga")
    sz = Sizes(length, slab_rows, groups)
    tb = tables(sz)
    lattice = orbitals.reshape(slab_rows, plane_cells)
    half = jnp.bfloat16
    counter = jnp.arange(length, dtype=jnp.int32)
    local_y = lax.axis_index("ga") * sz.cols + jnp.arange(sz.cols, dtype=jnp.int32)
    screen = screening(counter, local_y, counter, length) * retained.reshape(
        length, sz.cols, length
    ).astype(jnp.float32)
    screen = jnp.pad(screen.transpose(1, 0, 2), ((0, 0), (0, 0), (0, LANES - length)))

    flat = (slab_rows, plane_cells)
    lines = pltpu.VMEM((sz.pack, sz.quads * sz.rows, LANES), jnp.float32)
    mids = pltpu.VMEM((sz.pack, sz.groups * sz.inner * sz.cols, LANES), jnp.float32)
    sent = jax.ShapeDtypeStruct(sz.sent, half)

    def to_spectrum(visitors):
        send = pl.pallas_call(
            partial(forward_kernel, sz), out_shape=sent, scratch_shapes=[lines], name="forward"
        )(lattice, visitors, tb["z"], tb["y"])
        got = lax.all_to_all(send, "ga", split_axis=0, concat_axis=0, tiled=True)
        send, total = pl.pallas_call(
            partial(middle_kernel, sz),
            out_shape=(sent, jax.ShapeDtypeStruct((1, LANES), jnp.float32)),
            scratch_shapes=[mids, mids],
            name="middle",
        )(got, tb["x"], tb["xb"], screen)
        return lax.all_to_all(send, "ga", split_axis=0, concat_axis=0, tiled=True), jnp.sum(total)

    def crossed(got, visitors, running):
        return pl.pallas_call(
            partial(cross_kernel, sz),
            out_shape=(
                jax.ShapeDtypeStruct(flat, jnp.float32),
                jax.ShapeDtypeStruct(flat, half),
            ),
            scratch_shapes=[lines],
            name="crossed",
        )(got, lattice, visitors, running, tb["yb"], tb["zb"])

    band_reach = max(1, lax.axis_size("band") // 8)
    visitors = passed_along(lattice.astype(half), "band", 1)
    got, own_total = to_spectrum(lattice)
    running = pl.pallas_call(
        partial(own_kernel, sz),
        out_shape=jax.ShapeDtypeStruct(flat, jnp.float32),
        scratch_shapes=[lines],
        name="own",
    )(got, lattice, tb["yb"], tb["zb"])
    got, total = to_spectrum(visitors)
    running, carried = crossed(got, visitors, running)
    own_total = own_total + total

    def round_once(rounds_done, state):
        visitors, carried, carried_total, running, own_total = state
        visitors = passed_along(visitors, "band", 1)
        carried = passed_along(carried, "band", 1)
        carried_total = passed_along(carried_total, "band", 1)
        got, total = to_spectrum(visitors)
        running, added = crossed(got, visitors, running)
        carried = (carried.astype(jnp.float32) + added.astype(jnp.float32)).astype(half)
        return visitors, carried, carried_total + total, running, own_total + total

    state = (visitors, carried, total, running, own_total)
    if band_reach > 1:
        state = lax.fori_loop(1, band_reach, round_once, state)
    visitors, carried, total, running, own_total = state
    returned = passed_along(carried, "band", -band_reach)
    intersection = own_total + passed_along(total, "band", -band_reach)
    intersection = lax.psum(intersection, "ga") / float(length**3)
    running = running + returned.astype(jnp.float32)
    return (running.reshape(orbitals.shape), intersection.reshape(1, 1))


def solution(mesh):
    placed = (P("band", "ga", None), P(None, "ga"))
    return jax.shard_map(
        local,
        mesh=mesh,
        in_specs=placed,
        out_specs=(P("band", "ga", None), P("band", None)),
        check_vma=False,
    )
```

```python
import math
from functools import partial

import jax
import jax.numpy as jnp
import numpy as np
from jax import lax
from jax.experimental import pallas as pl
from jax.experimental.pallas import tpu as pltpu
from jax.sharding import PartitionSpec as P

LANES = 128


def passed_along(value, axis, steps):
    count = lax.axis_size(axis)
    pairs = [(source, (source + steps) % count) for source in range(count)]
    return lax.ppermute(value, axis, pairs)


def cas_table(length):
    counter = np.arange(length)
    angles = 2.0 * np.pi / length * (counter[:, None] * counter[None, :] % length)
    scaled = (np.cos(angles) + np.sin(angles)) / np.sqrt(float(length))
    return scaled.astype(np.float32).astype(jnp.bfloat16).astype(np.float32)


def wrapped(indices, length):
    return jnp.where(indices < length // 2, indices, indices - length).astype(jnp.float32)


def screening(rows_x, rows_y, rows_z, length):
    freq_x = wrapped(rows_x, length)
    freq_y = wrapped(rows_y, length)
    freq_z = wrapped(rows_z, length)
    squared = freq_x[:, None, None] ** 2 + freq_y[None, :, None] ** 2 + freq_z[None, None, :] ** 2
    spread = length / 4.0
    return 1.0 / (1.0 + squared / (spread * spread))


def lane_of(shape):
    return lax.broadcasted_iota(jnp.int32, shape, len(shape) - 1)


def dense(parts, length):
    spill = LANES - length
    lane = lane_of(parts[0].shape)
    last = parts[-1]
    return [
        jnp.where(lane < length, part, pltpu.roll(last, (length - spill * j) % LANES, last.ndim - 1))
        for j, part in enumerate(parts[:-1])
    ]


def undense(parts, length):
    spill = LANES - length
    lane = lane_of(parts[0].shape)
    last = jnp.zeros_like(parts[0])
    for j, part in enumerate(parts):
        moved = pltpu.roll(part, (spill * j - length) % LANES, part.ndim - 1)
        last = jnp.where((lane >= spill * j) & (lane < spill * (j + 1)), moved, last)
    return last


def dot(a, b):
    return jnp.dot(a, b, preferred_element_type=jnp.float32)


class Sizes:
    def __init__(self, length, rows, groups):
        self.length = length
        self.rows = rows
        self.groups = groups
        self.cols = length // groups
        whole = math.lcm(length, LANES)
        self.pack = whole // length
        self.chunks = whole // LANES
        self.quads = length // self.pack
        self.width = self.pack * length
        self.inner = rows // self.pack
        assert self.chunks == self.pack - 1 and self.inner % 2 == 0 and self.cols % 2 == 0
        assert groups & (groups - 1) == 0


def tables(sz):
    table = cas_table(sz.length)
    spread = np.zeros((sz.width, sz.pack * LANES), np.float32)
    for r in range(sz.pack):
        spread[r * sz.length:(r + 1) * sz.length, r * LANES:r * LANES + sz.length] = table
    y_order = np.arange(sz.length).reshape(sz.quads, sz.pack).T.reshape(-1)
    turned = []
    for me in range(sz.groups):
        peers = np.arange(sz.groups) ^ me
        freq = np.arange(sz.length).reshape(sz.groups, sz.cols)[peers].reshape(-1)
        x_all = np.arange(sz.length).reshape(sz.groups, sz.pack, sz.inner)[peers]
        x_order = x_all.transpose(1, 0, 2).reshape(-1)
        y = table[freq][:, y_order]
        x = table[:, x_order]
        turned.append(np.stack([y, y.T, x, x.T]))
    turned = jnp.asarray(np.stack(turned), jnp.bfloat16)
    mine = lax.dynamic_index_in_dim(turned, lax.axis_index("ga"), 0, keepdims=False)
    return jnp.asarray(spread, jnp.bfloat16), jnp.asarray(spread.T, jnp.bfloat16), mine


def pieces(row):
    rows, rest = [], row
    for _ in range(3):
        rows.append(rest.astype(jnp.bfloat16).astype(jnp.float32))
        rest = rest - rows[-1]
    at = lax.broadcasted_iota(jnp.int32, (8, LANES), 0)
    out = jnp.zeros((8, LANES), jnp.float32)
    for i, piece in enumerate(rows):
        out = jnp.where(at == i, piece, out)
    return out


def forward_kernel(sz, a_ref, b_ref, z_ref, t_ref, *refs):
    out_refs, s_ref = refs[:-1], refs[-1]
    w = sz.width
    rows = jnp.concatenate(
        [
            a_ref[:, q * w:(q + 1) * w] * b_ref[:, q * w:(q + 1) * w].astype(jnp.float32)
            for q in range(sz.quads)
        ],
        axis=0,
    ).astype(jnp.bfloat16)
    spread = dot(rows, z_ref[...])
    for r in range(sz.pack):
        s_ref[r] = spread[:, r * LANES:(r + 1) * LANES]
    y = t_ref[0]
    for xi in range(0, sz.inner, 2):
        planes = []
        for g in range(sz.pack):
            col = jnp.concatenate(
                [
                    jnp.concatenate(
                        [
                            s_ref[r, pl.ds(g * sz.inner + xi + h, sz.quads, stride=sz.rows), :]
                            for r in range(sz.pack)
                        ],
                        axis=0,
                    )
                    for h in range(2)
                ],
                axis=1,
            ).astype(jnp.bfloat16)
            planes.append(dot(y, col))
        packed = [
            dense([plane[:, h * LANES:(h + 1) * LANES] for plane in planes], sz.length)
            for h in range(2)
        ]
        for j in range(sz.chunks):
            for p in range(sz.groups):
                cut = slice(p * sz.cols, (p + 1) * sz.cols)
                out_refs[p][j, xi * sz.cols:(xi + 2) * sz.cols, :] = jnp.concatenate(
                    [packed[0][j][cut], packed[1][j][cut]], axis=0
                ).astype(jnp.bfloat16)


def middle_kernel(sz, *refs):
    n = sz.groups
    r_refs, (t_ref, screen_ref), out_refs, (f_ref, g_ref) = (
        refs[:n], refs[n:n + 2], refs[n + 2:2 * n + 2], refs[2 * n + 2:]
    )
    span = sz.inner * sz.cols
    for s in range(n):
        parts = [r_refs[s][j].astype(jnp.float32) for j in range(sz.chunks)]
        for g, part in enumerate(parts + [undense(parts, sz.length)]):
            f_ref[g, s * span:(s + 1) * span, :] = part
    many = n * sz.inner
    total = jnp.zeros((sz.length, LANES), jnp.float32)
    x, xb = t_ref[2], t_ref[3]
    for ky in range(0, sz.cols, 2):
        col = jnp.concatenate(
            [
                jnp.concatenate(
                    [f_ref[g, pl.ds(ky + h, many, stride=sz.cols), :] for g in range(sz.pack)],
                    axis=0,
                )
                for h in range(2)
            ],
            axis=1,
        ).astype(jnp.bfloat16)
        spectrum = dot(x, col).astype(jnp.bfloat16).astype(jnp.float32)
        screen = jnp.concatenate([screen_ref[ky], screen_ref[ky + 1]], axis=1)
        weighted = spectrum * screen
        energy = spectrum * weighted
        total = total + energy[:, :LANES] + energy[:, LANES:]
        back = dot(xb, weighted.astype(jnp.bfloat16))
        for h in range(2):
            for g in range(sz.pack):
                g_ref[g, pl.ds(ky + h, many, stride=sz.cols), :] = back[
                    g * many:(g + 1) * many, h * LANES:(h + 1) * LANES
                ]
    tail = pieces(jnp.sum(total, axis=0, keepdims=True))
    tail = jnp.concatenate([tail, jnp.zeros_like(tail)], axis=0).astype(jnp.bfloat16)
    for s in range(n):
        parts = [g_ref[g, s * span:(s + 1) * span, :] for g in range(sz.pack)]
        for j, part in enumerate(dense(parts, sz.length)):
            out_refs[s][j * span:(j + 1) * span, :] = part.astype(jnp.bfloat16)
        out_refs[s][sz.chunks * span:, :] = tail


def backward_body(sz, r_refs, zb_ref, t_ref, s_ref):
    span = sz.inner * sz.cols
    yb = t_ref[1]
    for xi in range(0, sz.inner, 2):
        blocks = []
        for p in range(sz.groups):
            parts = [
                r_refs[p][j * span + xi * sz.cols:j * span + (xi + 2) * sz.cols, :].astype(jnp.float32)
                for j in range(sz.chunks)
            ]
            blocks.append(parts + [undense(parts, sz.length)])
        for g in range(sz.pack):
            col = jnp.concatenate(
                [
                    jnp.concatenate(
                        [blocks[p][g][h * sz.cols:(h + 1) * sz.cols] for p in range(sz.groups)],
                        axis=0,
                    )
                    for h in range(2)
                ],
                axis=1,
            ).astype(jnp.bfloat16)
            plane = dot(yb, col)
            for h in range(2):
                for r in range(sz.pack):
                    s_ref[r, pl.ds(g * sz.inner + xi + h, sz.quads, stride=sz.rows), :] = plane[
                        r * sz.quads:(r + 1) * sz.quads, h * LANES:(h + 1) * LANES
                    ]
    total = sum(
        jnp.sum(r_refs[p][sz.chunks * span:, :].astype(jnp.float32), axis=0, keepdims=True)
        for p in range(sz.groups)
    )
    rows = jnp.concatenate([s_ref[r].astype(jnp.bfloat16) for r in range(sz.pack)], axis=1)
    return dot(rows, zb_ref[...]).astype(jnp.bfloat16).astype(jnp.float32), total


def own_kernel(sz, *refs):
    n = sz.groups
    r_refs, (a_ref, zb_ref, t_ref, out_ref, sum_ref, s_ref) = refs[:n], refs[n:]
    v, total = backward_body(sz, r_refs, zb_ref, t_ref, s_ref)
    sum_ref[...] = total
    for q in range(sz.quads):
        cut = slice(q * sz.width, (q + 1) * sz.width)
        out_ref[:, cut] = v[q * sz.rows:(q + 1) * sz.rows] * a_ref[:, cut]


def cross_kernel(sz, carrying, *refs):
    n = sz.groups
    r_refs, (a_ref, b_ref, run_ref, sum_in_ref), refs = refs[:n], refs[n:n + 4], refs[n + 4:]
    if carrying:
        carry_ref, refs = refs[0], refs[1:]
    zb_ref, t_ref, out_ref, sum_ref, back_ref, s_ref = refs
    v, total = backward_body(sz, r_refs, zb_ref, t_ref, s_ref)
    sum_ref[...] = sum_in_ref[...] + total
    cells = a_ref.shape[1]
    for q in range(sz.quads):
        cut = slice(q * sz.width, (q + 1) * sz.width)
        part = v[q * sz.rows:(q + 1) * sz.rows]
        out_ref[:, cut] = run_ref[:, cut] + part * b_ref[:, cut].astype(jnp.float32)
        back = part * a_ref[:, cut]
        if carrying:
            back = back + carry_ref[:, cut].astype(jnp.float32)
        back_ref[:, cut] = back.astype(back_ref.dtype)
    if carrying:
        total = total + jnp.sum(carry_ref[:, cells:].astype(jnp.float32), axis=0, keepdims=True)
    tail = pieces(total)
    rest = jnp.zeros((sz.rows - tail.shape[0], LANES), jnp.float32)
    back_ref[:, cells:] = jnp.concatenate([tail, rest], axis=0).astype(back_ref.dtype)


def last_kernel(sz, run_ref, sum_ref, got_ref, out_ref, block_ref):
    cells = run_ref.shape[1]
    out_ref[...] = run_ref[...] + got_ref[:, :cells].astype(jnp.float32)
    total = sum_ref[...] + jnp.sum(got_ref[:, cells:].astype(jnp.float32), axis=0, keepdims=True)
    block_ref[...] = jnp.sum(total, axis=1, keepdims=True) / float(sz.length**3)


def call(kernel, outs, args, scratch=(), name=None):
    held = [pltpu.with_memory_space_constraint(arg, pltpu.VMEM) for arg in args]
    return pl.pallas_call(
        kernel,
        out_shape=[pltpu.VMEM(shape, kind) for shape, kind in outs],
        in_specs=[pl.BlockSpec(memory_space=pltpu.VMEM)] * len(args),
        out_specs=[pl.BlockSpec(memory_space=pltpu.VMEM)] * len(outs),
        scratch_shapes=list(scratch),
        compiler_params=pltpu.CompilerParams(vmem_limit_bytes=24 * 2**20),
        name=name,
    )(*held)


def exchange(blocks):
    count = len(blocks)
    got = [blocks[0]]
    for k in range(1, count):
        got.append(lax.ppermute(blocks[k], "ga", [(d, d ^ k) for d in range(count)]))
    return got


def local(orbitals, retained):
    bands_dev, slab_rows, plane_cells = orbitals.shape
    assert bands_dev == 1
    length = retained.shape[0]
    groups = lax.axis_size("ga")
    sz = Sizes(length, slab_rows, groups)
    z, zb, mine = tables(sz)
    lattice = orbitals.reshape(slab_rows, plane_cells)
    half, full = jnp.bfloat16, jnp.float32
    counter = jnp.arange(length, dtype=jnp.int32)
    local_y = lax.axis_index("ga") * sz.cols + jnp.arange(sz.cols, dtype=jnp.int32)
    screen = screening(counter, local_y, counter, length) * retained.reshape(
        length, sz.cols, length
    ).astype(jnp.float32)
    screen = jnp.pad(screen.transpose(1, 0, 2), ((0, 0), (0, 0), (0, LANES - length)))

    flat = (slab_rows, plane_cells)
    wide = (slab_rows, plane_cells + LANES)
    span = sz.inner * sz.cols
    lines = pltpu.VMEM((sz.pack, sz.quads * sz.rows, LANES), full)
    mids = pltpu.VMEM((sz.pack, groups * span, LANES), full)
    there = [((sz.chunks, span, LANES), half)] * groups
    again = [((sz.chunks * span + 16, LANES), half)] * groups

    def to_potential(visitors):
        sent = call(
            partial(forward_kernel, sz), there, [lattice, visitors, z, mine], [lines], "forward"
        )
        sent = call(
            partial(middle_kernel, sz), again, exchange(sent) + [mine, screen], [mids, mids], "middle"
        )
        return exchange(sent)

    def crossed(got, visitors, running, total, carried):
        return call(
            partial(cross_kernel, sz, len(carried) > 0),
            [(flat, full), ((1, LANES), full), (wide, half)],
            got + [lattice, visitors, running, total] + carried + [zb, mine],
            [lines],
            "crossed",
        )

    band_reach = max(1, lax.axis_size("band") // 8)
    visitors = passed_along(lattice.astype(half), "band", 1)
    running, total = call(
        partial(own_kernel, sz),
        [(flat, full), ((1, LANES), full)],
        to_potential(lattice) + [lattice, zb, mine],
        [lines],
        "own",
    )
    running, total, carried = crossed(to_potential(visitors), visitors, running, total, [])

    def round_once(rounds_done, state):
        visitors, carried, running, total = state
        visitors = passed_along(visitors, "band", 1)
        carried = passed_along(carried, "band", 1)
        running, total, carried = crossed(
            to_potential(visitors), visitors, running, total, [carried]
        )
        return visitors, carried, running, total

    if band_reach > 1:
        state = (visitors, carried, running, total)
        visitors, carried, running, total = lax.fori_loop(1, band_reach, round_once, state)
    returned = passed_along(carried, "band", -band_reach)
    field, block = pl.pallas_call(
        partial(last_kernel, sz),
        out_shape=[jax.ShapeDtypeStruct(flat, full), jax.ShapeDtypeStruct((1, 1), full)],
        compiler_params=pltpu.CompilerParams(vmem_limit_bytes=24 * 2**20),
        name="last",
    )(*[pltpu.with_memory_space_constraint(v, pltpu.VMEM) for v in (running, total, returned)])
    return field.reshape(orbitals.shape), block


def solution(mesh):
    placed = (P("band", "ga", None), P(None, "ga"))
    return jax.shard_map(
        local,
        mesh=mesh,
        in_specs=placed,
        out_specs=(P("band", "ga", None), P("band", None)),
        check_vma=False,
    )
```

```python
import math
from functools import partial

import jax
import jax.numpy as jnp
import numpy as np
from jax import lax
from jax.experimental import pallas as pl
from jax.experimental.pallas import tpu as pltpu
from jax.sharding import PartitionSpec as P

LANES = 128


def passed_along(value, axis, steps):
    count = lax.axis_size(axis)
    pairs = [(source, (source + steps) % count) for source in range(count)]
    return lax.ppermute(value, axis, pairs)


def cas_table(length):
    counter = np.arange(length)
    angles = 2.0 * np.pi / length * (counter[:, None] * counter[None, :] % length)
    scaled = (np.cos(angles) + np.sin(angles)) / np.sqrt(float(length))
    return scaled.astype(np.float32).astype(jnp.bfloat16).astype(np.float32)


def wrapped(indices, length):
    return jnp.where(indices < length // 2, indices, indices - length).astype(jnp.float32)


def screening(rows_x, rows_y, rows_z, length):
    freq_x = wrapped(rows_x, length)
    freq_y = wrapped(rows_y, length)
    freq_z = wrapped(rows_z, length)
    squared = freq_x[:, None, None] ** 2 + freq_y[None, :, None] ** 2 + freq_z[None, None, :] ** 2
    spread = length / 4.0
    return 1.0 / (1.0 + squared / (spread * spread))


def lane_of(shape):
    return lax.broadcasted_iota(jnp.int32, shape, len(shape) - 1)


def dense(parts, length):
    spill = LANES - length
    lane = lane_of(parts[0].shape)
    last = parts[-1]
    return [
        jnp.where(lane < length, part, pltpu.roll(last, (length - spill * j) % LANES, last.ndim - 1))
        for j, part in enumerate(parts[:-1])
    ]


def undense(parts, length):
    spill = LANES - length
    lane = lane_of(parts[0].shape)
    last = jnp.zeros_like(parts[0])
    for j, part in enumerate(parts):
        moved = pltpu.roll(part, (spill * j - length) % LANES, part.ndim - 1)
        last = jnp.where((lane >= spill * j) & (lane < spill * (j + 1)), moved, last)
    return last


def dot(a, b):
    return jnp.dot(a, b, preferred_element_type=jnp.float32)


class Sizes:
    def __init__(self, length, slab, groups, start, rows):
        self.length = length
        self.slab = slab
        self.start = start
        self.rows = rows
        self.groups = groups
        self.cols = length // groups
        whole = math.lcm(length, LANES)
        self.pack = whole // length
        self.chunks = whole // LANES
        self.quads = length // self.pack
        self.width = self.pack * length
        self.inner = rows // self.pack
        self.span = self.inner * self.cols
        assert self.chunks == self.pack - 1 and self.inner % 2 == 0 and self.cols % 2 == 0
        assert groups & (groups - 1) == 0


def tables(plans):
    sz = plans[0][0]
    table = cas_table(sz.length)
    spread = np.zeros((sz.width, sz.pack * LANES), np.float32)
    for r in range(sz.pack):
        spread[r * sz.length:(r + 1) * sz.length, r * LANES:r * LANES + sz.length] = table
    y_order = np.arange(sz.length).reshape(sz.quads, sz.pack).T.reshape(-1)
    turned = []
    for me in range(sz.groups):
        peers = np.arange(sz.groups) ^ me
        freq = np.arange(sz.length).reshape(sz.groups, sz.cols)[peers].reshape(-1)
        y = table[freq][:, y_order]
        found = [y, y.T]
        for plan in plans:
            x_order = []
            for cut in plan:
                inside = cut.start + np.arange(cut.rows).reshape(cut.pack, 1, cut.inner)
                x_order.append((inside + peers.reshape(1, -1, 1) * cut.slab).reshape(-1))
            x = table[:, np.concatenate(x_order)]
            found += [x, x.T]
        turned.append(np.stack(found))
    turned = jnp.asarray(np.stack(turned), jnp.bfloat16)
    mine = lax.dynamic_index_in_dim(turned, lax.axis_index("ga"), 0, keepdims=False)
    return jnp.asarray(spread, jnp.bfloat16), jnp.asarray(spread.T, jnp.bfloat16), mine


def pieces(row):
    rows, rest = [], row
    for _ in range(3):
        rows.append(rest.astype(jnp.bfloat16).astype(jnp.float32))
        rest = rest - rows[-1]
    at = lax.broadcasted_iota(jnp.int32, (8, LANES), 0)
    out = jnp.zeros((8, LANES), jnp.float32)
    for i, piece in enumerate(rows):
        out = jnp.where(at == i, piece, out)
    return out


def forward_kernel(sz, a_ref, b_ref, z_ref, t_ref, *refs):
    out_refs, s_ref = refs[:-1], refs[-1]
    w = sz.width
    rows = jnp.concatenate(
        [
            a_ref[sz.start:sz.start + sz.rows, q * w:(q + 1) * w]
            * b_ref[:, q * w:(q + 1) * w].astype(jnp.float32)
            for q in range(sz.quads)
        ],
        axis=0,
    ).astype(jnp.bfloat16)
    spread = dot(rows, z_ref[...])
    for r in range(sz.pack):
        s_ref[r] = spread[:, r * LANES:(r + 1) * LANES]
    y = t_ref[0]
    for xi in range(0, sz.inner, 2):
        planes = []
        for g in range(sz.pack):
            col = jnp.concatenate(
                [
                    jnp.concatenate(
                        [
                            s_ref[r, pl.ds(g * sz.inner + xi + h, sz.quads, stride=sz.rows), :]
                            for r in range(sz.pack)
                        ],
                        axis=0,
                    )
                    for h in range(2)
                ],
                axis=1,
            ).astype(jnp.bfloat16)
            planes.append(dot(y, col))
        packed = [
            dense([plane[:, h * LANES:(h + 1) * LANES] for plane in planes], sz.length)
            for h in range(2)
        ]
        for j in range(sz.chunks):
            for p in range(sz.groups):
                cut = slice(p * sz.cols, (p + 1) * sz.cols)
                out_refs[p][j, xi * sz.cols:(xi + 2) * sz.cols, :] = jnp.concatenate(
                    [packed[0][j][cut], packed[1][j][cut]], axis=0
                ).astype(jnp.bfloat16)


def middle_kernel(plan, which, *refs):
    sz, n, count = plan[0], plan[0].groups, len(plan)
    r_refs, refs = refs[:n * count], refs[n * count:]
    (t_ref, screen_ref), refs = refs[:2], refs[2:]
    out_refs, refs = refs[:n * count], refs[n * count:]
    f_refs, g_refs = refs[:count], refs[count:]
    for c, cut in enumerate(plan):
        for s in range(n):
            parts = [r_refs[c * n + s][j].astype(jnp.float32) for j in range(sz.chunks)]
            for g, part in enumerate(parts + [undense(parts, sz.length)]):
                f_refs[c][g, s * cut.span:(s + 1) * cut.span, :] = part
    total = jnp.zeros((sz.length, LANES), jnp.float32)
    x, xb = t_ref[2 + 2 * which], t_ref[3 + 2 * which]
    for ky in range(0, sz.cols, 2):
        col = jnp.concatenate(
            [
                jnp.concatenate(
                    [
                        f_refs[c][g, pl.ds(ky + h, n * cut.inner, stride=sz.cols), :]
                        for c, cut in enumerate(plan)
                        for g in range(sz.pack)
                    ],
                    axis=0,
                )
                for h in range(2)
            ],
            axis=1,
        ).astype(jnp.bfloat16)
        spectrum = dot(x, col).astype(jnp.bfloat16).astype(jnp.float32)
        screen = jnp.concatenate([screen_ref[ky], screen_ref[ky + 1]], axis=1)
        weighted = spectrum * screen
        energy = spectrum * weighted
        total = total + energy[:, :LANES] + energy[:, LANES:]
        back = dot(xb, weighted.astype(jnp.bfloat16))
        for h in range(2):
            at = 0
            for c, cut in enumerate(plan):
                many = n * cut.inner
                for g in range(sz.pack):
                    g_refs[c][g, pl.ds(ky + h, many, stride=sz.cols), :] = back[
                        at:at + many, h * LANES:(h + 1) * LANES
                    ]
                    at += many
    tail = pieces(jnp.sum(total, axis=0, keepdims=True))
    tail = jnp.concatenate([tail, jnp.zeros_like(tail)], axis=0).astype(jnp.bfloat16)
    for c, cut in enumerate(plan):
        for s in range(n):
            parts = [g_refs[c][g, s * cut.span:(s + 1) * cut.span, :] for g in range(sz.pack)]
            out_ref = out_refs[c * n + s]
            for j, part in enumerate(dense(parts, sz.length)):
                out_ref[j * cut.span:(j + 1) * cut.span, :] = part.astype(jnp.bfloat16)
            if cut.start == 0:
                out_ref[sz.chunks * cut.span:, :] = tail


def backward_body(sz, r_refs, zb_ref, t_ref, s_ref):
    span = sz.inner * sz.cols
    yb = t_ref[1]
    for xi in range(0, sz.inner, 2):
        blocks = []
        for p in range(sz.groups):
            parts = [
                r_refs[p][j * span + xi * sz.cols:j * span + (xi + 2) * sz.cols, :].astype(jnp.float32)
                for j in range(sz.chunks)
            ]
            blocks.append(parts + [undense(parts, sz.length)])
        for g in range(sz.pack):
            col = jnp.concatenate(
                [
                    jnp.concatenate(
                        [blocks[p][g][h * sz.cols:(h + 1) * sz.cols] for p in range(sz.groups)],
                        axis=0,
                    )
                    for h in range(2)
                ],
                axis=1,
            ).astype(jnp.bfloat16)
            plane = dot(yb, col)
            for h in range(2):
                for r in range(sz.pack):
                    s_ref[r, pl.ds(g * sz.inner + xi + h, sz.quads, stride=sz.rows), :] = plane[
                        r * sz.quads:(r + 1) * sz.quads, h * LANES:(h + 1) * LANES
                    ]
    total = None
    if sz.start == 0:
        total = sum(
            jnp.sum(r_refs[p][sz.chunks * span:, :].astype(jnp.float32), axis=0, keepdims=True)
            for p in range(sz.groups)
        )
    rows = jnp.concatenate([s_ref[r].astype(jnp.bfloat16) for r in range(sz.pack)], axis=1)
    return dot(rows, zb_ref[...]).astype(jnp.bfloat16).astype(jnp.float32), total


def own_kernel(sz, plan, *refs):
    n = sz.groups
    r_refs, refs = refs[:n], refs[n:]
    part_refs, refs = refs[:len(plan)], refs[len(plan):]
    a_ref, sum_in_ref, zb_ref, t_ref, out_ref, sum_ref, s_ref = refs
    v, total = backward_body(sz, r_refs, zb_ref, t_ref, s_ref)
    sum_ref[...] = total + sum_in_ref[...]
    for q in range(sz.quads):
        lanes = slice(q * sz.width, (q + 1) * sz.width)
        own = v[q * sz.rows:(q + 1) * sz.rows]
        for cut, part_ref in zip(plan, part_refs):
            rows = slice(cut.start, cut.start + cut.rows)
            out_ref[rows, lanes] = own[rows] * a_ref[rows, lanes] + part_ref[:, lanes]


def cross_kernel(sz, again, *refs):
    n = sz.groups
    first = sz.start == 0
    r_refs, refs = refs[:n], refs[n:]
    a_ref, b_ref, zb_ref, t_ref = refs[:4]
    refs = refs[4:]
    if again:
        run_ref, carry_ref = refs[:2]
        refs = refs[2:]
        if first:
            sum_in_ref, refs = refs[0], refs[1:]
    out_ref, back_ref, s_ref = refs[0], refs[1], refs[-1]
    v, total = backward_body(sz, r_refs, zb_ref, t_ref, s_ref)
    cells = a_ref.shape[1]
    rows = slice(sz.start, sz.start + sz.rows)
    for q in range(sz.quads):
        lanes = slice(q * sz.width, (q + 1) * sz.width)
        part = v[q * sz.rows:(q + 1) * sz.rows]
        out = part * b_ref[:, lanes].astype(jnp.float32)
        back = part * a_ref[rows, lanes]
        if again:
            out = out + run_ref[:, lanes]
            back = back + carry_ref[:, lanes].astype(jnp.float32)
        out_ref[:, lanes] = out
        back_ref[:, lanes] = back.astype(back_ref.dtype)
    if first:
        sum_ref = refs[2]
        sum_ref[...] = total + sum_in_ref[...] if again else total
        if again:
            carried = carry_ref[:, cells:].astype(jnp.float32)
            total = total + jnp.sum(carried, axis=0, keepdims=True)
        tail = pieces(total)
        if sz.rows > tail.shape[0]:
            rest = jnp.zeros((sz.rows - tail.shape[0], LANES), jnp.float32)
            tail = jnp.concatenate([tail, rest], axis=0)
        back_ref[:, cells:] = tail.astype(back_ref.dtype)


def last_kernel(sz, plan, run_ref, sum_ref, *refs):
    got_refs, (out_ref, block_ref) = refs[:len(plan)], refs[len(plan):]
    cells = run_ref.shape[1]
    total = sum_ref[...]
    for cut, got_ref in zip(plan, got_refs):
        rows = slice(cut.start, cut.start + cut.rows)
        out_ref[rows] = run_ref[rows] + got_ref[:, :cells].astype(jnp.float32)
        if cut.start == 0:
            carried = got_ref[:, cells:].astype(jnp.float32)
            total = total + jnp.sum(carried, axis=0, keepdims=True)
    block_ref[...] = jnp.sum(total, axis=1, keepdims=True) / float(sz.length**3)


def call(kernel, outs, args, scratch=()):
    held = [pltpu.with_memory_space_constraint(arg, pltpu.VMEM) for arg in args]
    return pl.pallas_call(
        kernel,
        out_shape=[pltpu.VMEM(shape, kind) for shape, kind in outs],
        in_specs=[pl.BlockSpec(memory_space=pltpu.VMEM)] * len(args),
        out_specs=[pl.BlockSpec(memory_space=pltpu.VMEM)] * len(outs),
        scratch_shapes=list(scratch),
        compiler_params=pltpu.CompilerParams(vmem_limit_bytes=24 * 2**20),
    )(*held)


def after(value, before):
    return value if before is None else lax.optimization_barrier((value, before))[0]


def exchange(blocks):
    count = len(blocks)
    got = {0: blocks[0]}
    for k in range(count - 1, 0, -1):
        got[k] = lax.ppermute(blocks[k], "ga", [(d, d ^ k) for d in range(count)])
    return [got[k] for k in range(count)]


def chunk_rows(rows):
    least = 8
    return [rows - least, least] if rows > least else [rows]


def local(orbitals, retained):
    bands_dev, slab_rows, plane_cells = orbitals.shape
    assert bands_dev == 1
    length = retained.shape[0]
    groups = lax.axis_size("ga")
    sz = Sizes(length, slab_rows, groups, 0, slab_rows)
    plan, at = [], 0
    for rows in chunk_rows(slab_rows):
        plan.append(Sizes(length, slab_rows, groups, at, rows))
        at += rows
    z, zb, mine = tables([[sz], plan])
    lattice = orbitals.reshape(slab_rows, plane_cells)
    half, full = jnp.bfloat16, jnp.float32
    counter = jnp.arange(length, dtype=jnp.int32)
    local_y = lax.axis_index("ga") * sz.cols + jnp.arange(sz.cols, dtype=jnp.int32)
    screen = screening(counter, local_y, counter, length) * retained.reshape(
        length, sz.cols, length
    ).astype(jnp.float32)
    screen = jnp.pad(screen.transpose(1, 0, 2), ((0, 0), (0, 0), (0, LANES - length)))

    flat = (slab_rows, plane_cells)

    def lines(cut):
        return pltpu.VMEM((cut.pack, cut.quads * cut.rows, LANES), full)

    def mids(cut):
        return pltpu.VMEM((cut.pack, groups * cut.span, LANES), full)

    def forward(cut, visitors):
        there = [((cut.chunks, cut.span, LANES), half)] * groups
        kernel = partial(forward_kernel, cut)
        return call(kernel, there, [lattice, visitors, z, mine], [lines(cut)])

    def middle(cuts, which, got):
        outs = []
        for cut in cuts:
            tail = 16 if cut.start == 0 else 0
            outs += [((cut.chunks * cut.span + tail, LANES), half)] * groups
        scratch = [mids(cut) for cut in cuts] * 2
        kernel = partial(middle_kernel, cuts, which)
        sent = call(kernel, outs, got + [mine, screen], scratch)
        return [sent[c * groups:(c + 1) * groups] for c in range(len(cuts))]

    def crossed(cut, got, visitors, old):
        first = cut.start == 0
        outs = [
            ((cut.rows, plane_cells), full),
            ((cut.rows, plane_cells + (LANES if first else 0)), half),
        ]
        if first:
            outs.append(((1, LANES), full))
        kernel = partial(cross_kernel, cut, len(old) > 0)
        return call(kernel, outs, got + [lattice, visitors, zb, mine] + old, [lines(cut)])

    def pair(visitors, old, ahead=None):
        got, before = [], None
        for c, cut in enumerate(plan):
            before = forward(cut, after(visitors[c], before))
            got += exchange(before)
        got = after(got, ahead)
        sent = middle(plan, 1, got)
        fresh = [None] * len(plan)
        for c in reversed(range(len(plan))):
            fresh[c] = crossed(plan[c], exchange(sent[c]), visitors[c], old[c])
        return [part[0] for part in fresh], [part[1] for part in fresh], fresh[0][2]

    band_reach = max(1, lax.axis_size("band") // 8)
    visitors = []
    for cut in plan:
        chunk = lattice[cut.start:cut.start + cut.rows].astype(half)
        visitors.append(passed_along(chunk, "band", 1))
    sent = forward(sz, lattice)
    visitors = [after(chunk, sent) for chunk in visitors]
    sent = middle([sz], 0, exchange(sent))[0]
    running, carried, total = pair(visitors, [[]] * len(plan), sent)

    def round_once(rounds_done, state):
        visitors, running, carried, total = state
        visitors = [passed_along(chunk, "band", 1) for chunk in visitors]
        carried = [passed_along(chunk, "band", 1) for chunk in carried]
        old = [list(both) for both in zip(running, carried)]
        old[0].append(total)
        running, carried, total = pair(visitors, old)
        return visitors, running, carried, total

    if band_reach > 1:
        state = (visitors, running, carried, total)
        visitors, running, carried, total = lax.fori_loop(1, band_reach, round_once, state)
    returned = []
    for chunk in carried:
        returned.append(passed_along(chunk, "band", -band_reach))
    sent = after(sent, total)
    running, total = call(
        partial(own_kernel, sz, plan),
        [(flat, full), ((1, LANES), full)],
        exchange(sent) + running + [lattice, total, zb, mine],
        [lines(sz)],
    )
    field, block = pl.pallas_call(
        partial(last_kernel, sz, plan),
        out_shape=[jax.ShapeDtypeStruct(flat, full), jax.ShapeDtypeStruct((1, 1), full)],
        compiler_params=pltpu.CompilerParams(vmem_limit_bytes=24 * 2**20),
        name="last",
    )(*[pltpu.with_memory_space_constraint(v, pltpu.VMEM) for v in [running, total] + returned])
    return field.reshape(orbitals.shape), block


def solution(mesh):
    placed = (P("band", "ga", None), P(None, "ga"))

    return jax.shard_map(
        local,
        mesh=mesh,
        in_specs=placed,
        out_specs=(P("band", "ga", None), P("band", None)),
        check_vma=False,
    )
```

```python
import math
from functools import partial

import jax
import jax.numpy as jnp
import numpy as np
from jax import lax
from jax.experimental import pallas as pl
from jax.experimental.pallas import tpu as pltpu
from jax.sharding import PartitionSpec as P

LANES = 128


def passed_along(value, axis, steps):
    count = lax.axis_size(axis)
    pairs = [(source, (source + steps) % count) for source in range(count)]
    return lax.ppermute(value, axis, pairs)


def cas_table(length):
    counter = np.arange(length)
    angles = 2.0 * np.pi / length * (counter[:, None] * counter[None, :] % length)
    scaled = (np.cos(angles) + np.sin(angles)) / np.sqrt(float(length))
    return scaled.astype(np.float32).astype(jnp.bfloat16).astype(np.float32)


def wrapped(indices, length):
    return jnp.where(indices < length // 2, indices, indices - length).astype(jnp.float32)


def lane_of(shape):
    return lax.broadcasted_iota(jnp.int32, shape, len(shape) - 1)


def dense(parts, length):
    spill = LANES - length
    lane = lane_of(parts[0].shape)
    last = parts[-1]
    return [
        jnp.where(lane < length, part, pltpu.roll(last, (length - spill * j) % LANES, last.ndim - 1))
        for j, part in enumerate(parts[:-1])
    ]


def undense(parts, length):
    spill = LANES - length
    lane = lane_of(parts[0].shape)
    last = jnp.zeros_like(parts[0])
    for j, part in enumerate(parts):
        moved = pltpu.roll(part, (spill * j - length) % LANES, part.ndim - 1)
        last = jnp.where((lane >= spill * j) & (lane < spill * (j + 1)), moved, last)
    return last


def dot(a, b):
    return jnp.dot(a, b, preferred_element_type=jnp.float32)


class Sizes:
    def __init__(self, length, slab, groups, start, rows):
        self.length = length
        self.slab = slab
        self.start = start
        self.rows = rows
        self.groups = groups
        self.cols = length // groups
        whole = math.lcm(length, LANES)
        self.pack = whole // length
        self.chunks = whole // LANES
        self.quads = length // self.pack
        self.width = self.pack * length
        self.inner = rows // self.pack
        self.span = self.inner * self.cols
        assert self.chunks == self.pack - 1 and self.inner % 2 == 0 and self.cols % 2 == 0
        assert groups & (groups - 1) == 0


def tables(plans):
    sz = plans[0][0]
    table = cas_table(sz.length)
    spread = np.zeros((sz.width, sz.pack * LANES), np.float32)
    for r in range(sz.pack):
        spread[r * sz.length:(r + 1) * sz.length, r * LANES:r * LANES + sz.length] = table
    y_order = np.arange(sz.length).reshape(sz.quads, sz.pack).T.reshape(-1)
    turned = []
    for me in range(sz.groups):
        peers = np.arange(sz.groups) ^ me
        freq = np.arange(sz.length).reshape(sz.groups, sz.cols)[peers].reshape(-1)
        y = table[freq][:, y_order]
        found = [y, y.T]
        for plan in plans:
            x_order = []
            for cut in plan:
                inside = cut.start + np.arange(cut.rows).reshape(cut.pack, 1, cut.inner)
                x_order.append((inside + peers.reshape(1, -1, 1) * cut.slab).reshape(-1))
            x = table[:, np.concatenate(x_order)]
            found += [x, x.T]
        turned.append(np.stack(found))
    turned = jnp.asarray(np.stack(turned), jnp.bfloat16)
    mine = lax.dynamic_index_in_dim(turned, lax.axis_index("ga"), 0, keepdims=False)
    return jnp.asarray(spread, jnp.bfloat16), jnp.asarray(spread.T, jnp.bfloat16), mine


def pieces(row):
    rows, rest = [], row
    for _ in range(3):
        rows.append(rest.astype(jnp.bfloat16).astype(jnp.float32))
        rest = rest - rows[-1]
    at = lax.broadcasted_iota(jnp.int32, (8, LANES), 0)
    out = jnp.zeros((8, LANES), jnp.float32)
    for i, piece in enumerate(rows):
        out = jnp.where(at == i, piece, out)
    return out


def split_kernel(plan, a_ref, *out_refs):
    for cut, out_ref in zip(plan, out_refs):
        out_ref[...] = a_ref[cut.start:cut.start + cut.rows, :].astype(out_ref.dtype)


def screen_kernel(sz, kept_ref, y_ref, out_ref):
    shape = (sz.length, LANES)
    lane = lane_of(shape)
    freq_x = wrapped(lax.broadcasted_iota(jnp.int32, shape, 0), sz.length)
    freq_z = wrapped(lane, sz.length)
    plane_x, plane_z = freq_x * freq_x, freq_z * freq_z
    spread = sz.length / 4.0
    for ky in range(sz.cols):
        at, off = divmod(ky * sz.length, LANES)
        turn = (LANES - off) % LANES
        kept = kept_ref[:, at * LANES:(at + 1) * LANES].astype(jnp.float32)
        if turn:
            kept = pltpu.roll(kept, turn, 1)
        if off + sz.length > LANES:
            more = kept_ref[:, (at + 1) * LANES:(at + 2) * LANES].astype(jnp.float32)
            kept = jnp.where(lane < LANES - off, kept, pltpu.roll(more, turn, 1))
        squared = plane_x + y_ref[ky] + plane_z
        screen = 1.0 / (1.0 + squared / (spread * spread)) * kept
        out_ref[ky] = jnp.where(lane < sz.length, screen, 0.0)


def forward_kernel(sz, a_ref, b_ref, z_ref, t_ref, *refs):
    out_refs, s_ref = refs[:-1], refs[-1]
    w = sz.width
    rows = jnp.concatenate(
        [
            a_ref[sz.start:sz.start + sz.rows, q * w:(q + 1) * w]
            * b_ref[:, q * w:(q + 1) * w].astype(jnp.float32)
            for q in range(sz.quads)
        ],
        axis=0,
    ).astype(jnp.bfloat16)
    spread = dot(rows, z_ref[...])
    for r in range(sz.pack):
        s_ref[r] = spread[:, r * LANES:(r + 1) * LANES]
    y = t_ref[0]
    for xi in range(0, sz.inner, 2):
        planes = []
        for g in range(sz.pack):
            col = jnp.concatenate(
                [
                    jnp.concatenate(
                        [
                            s_ref[r, pl.ds(g * sz.inner + xi + h, sz.quads, stride=sz.rows), :]
                            for r in range(sz.pack)
                        ],
                        axis=0,
                    )
                    for h in range(2)
                ],
                axis=1,
            ).astype(jnp.bfloat16)
            planes.append(dot(y, col))
        packed = [
            dense([plane[:, h * LANES:(h + 1) * LANES] for plane in planes], sz.length)
            for h in range(2)
        ]
        for j in range(sz.chunks):
            for p in range(sz.groups):
                cut = slice(p * sz.cols, (p + 1) * sz.cols)
                out_refs[p][j, xi * sz.cols:(xi + 2) * sz.cols, :] = jnp.concatenate(
                    [packed[0][j][cut], packed[1][j][cut]], axis=0
                ).astype(jnp.bfloat16)


def middle_kernel(plan, which, *refs):
    sz, n, count = plan[0], plan[0].groups, len(plan)
    r_refs, refs = refs[:n * count], refs[n * count:]
    (t_ref, screen_ref), refs = refs[:2], refs[2:]
    out_refs, refs = refs[:n * count], refs[n * count:]
    f_refs, g_refs = refs[:count], refs[count:]
    for c, cut in enumerate(plan):
        for s in range(n):
            parts = [r_refs[c * n + s][j].astype(jnp.float32) for j in range(sz.chunks)]
            for g, part in enumerate(parts + [undense(parts, sz.length)]):
                f_refs[c][g, s * cut.span:(s + 1) * cut.span, :] = part
    total = jnp.zeros((sz.length, LANES), jnp.float32)
    x, xb = t_ref[2 + 2 * which], t_ref[3 + 2 * which]
    for ky in range(0, sz.cols, 2):
        col = jnp.concatenate(
            [
                jnp.concatenate(
                    [
                        f_refs[c][g, pl.ds(ky + h, n * cut.inner, stride=sz.cols), :]
                        for c, cut in enumerate(plan)
                        for g in range(sz.pack)
                    ],
                    axis=0,
                )
                for h in range(2)
            ],
            axis=1,
        ).astype(jnp.bfloat16)
        spectrum = dot(x, col).astype(jnp.bfloat16).astype(jnp.float32)
        screen = jnp.concatenate([screen_ref[ky], screen_ref[ky + 1]], axis=1)
        weighted = spectrum * screen
        energy = spectrum * weighted
        total = total + energy[:, :LANES] + energy[:, LANES:]
        back = dot(xb, weighted.astype(jnp.bfloat16))
        for h in range(2):
            at = 0
            for c, cut in enumerate(plan):
                many = n * cut.inner
                for g in range(sz.pack):
                    g_refs[c][g, pl.ds(ky + h, many, stride=sz.cols), :] = back[
                        at:at + many, h * LANES:(h + 1) * LANES
                    ]
                    at += many
    tail = pieces(jnp.sum(total, axis=0, keepdims=True))
    tail = jnp.concatenate([tail, jnp.zeros_like(tail)], axis=0).astype(jnp.bfloat16)
    for c, cut in enumerate(plan):
        for s in range(n):
            parts = [g_refs[c][g, s * cut.span:(s + 1) * cut.span, :] for g in range(sz.pack)]
            out_ref = out_refs[c * n + s]
            for j, part in enumerate(dense(parts, sz.length)):
                out_ref[j * cut.span:(j + 1) * cut.span, :] = part.astype(jnp.bfloat16)
            if cut.start == 0:
                out_ref[sz.chunks * cut.span:, :] = tail


def backward_body(sz, r_refs, zb_ref, t_ref, s_ref):
    span = sz.inner * sz.cols
    yb = t_ref[1]
    for xi in range(0, sz.inner, 2):
        blocks = []
        for p in range(sz.groups):
            parts = [
                r_refs[p][j * span + xi * sz.cols:j * span + (xi + 2) * sz.cols, :].astype(jnp.float32)
                for j in range(sz.chunks)
            ]
            blocks.append(parts + [undense(parts, sz.length)])
        for g in range(sz.pack):
            col = jnp.concatenate(
                [
                    jnp.concatenate(
                        [blocks[p][g][h * sz.cols:(h + 1) * sz.cols] for p in range(sz.groups)],
                        axis=0,
                    )
                    for h in range(2)
                ],
                axis=1,
            ).astype(jnp.bfloat16)
            plane = dot(yb, col)
            for h in range(2):
                for r in range(sz.pack):
                    s_ref[r, pl.ds(g * sz.inner + xi + h, sz.quads, stride=sz.rows), :] = plane[
                        r * sz.quads:(r + 1) * sz.quads, h * LANES:(h + 1) * LANES
                    ]
    total = None
    if sz.start == 0:
        total = sum(
            jnp.sum(r_refs[p][sz.chunks * span:, :].astype(jnp.float32), axis=0, keepdims=True)
            for p in range(sz.groups)
        )
    rows = jnp.concatenate([s_ref[r].astype(jnp.bfloat16) for r in range(sz.pack)], axis=1)
    return dot(rows, zb_ref[...]).astype(jnp.bfloat16).astype(jnp.float32), total


def own_kernel(sz, plan, *refs):
    n = sz.groups
    r_refs, refs = refs[:n], refs[n:]
    part_refs, refs = refs[:len(plan)], refs[len(plan):]
    a_ref, sum_in_ref, zb_ref, t_ref, out_ref, sum_ref, s_ref = refs
    v, total = backward_body(sz, r_refs, zb_ref, t_ref, s_ref)
    sum_ref[...] = total + sum_in_ref[...]
    for q in range(sz.quads):
        lanes = slice(q * sz.width, (q + 1) * sz.width)
        own = v[q * sz.rows:(q + 1) * sz.rows]
        for cut, part_ref in zip(plan, part_refs):
            rows = slice(cut.start, cut.start + cut.rows)
            out_ref[rows, lanes] = own[rows] * a_ref[rows, lanes] + part_ref[:, lanes]


def cross_kernel(sz, again, *refs):
    n = sz.groups
    first = sz.start == 0
    r_refs, refs = refs[:n], refs[n:]
    a_ref, b_ref, zb_ref, t_ref = refs[:4]
    refs = refs[4:]
    if again:
        run_ref, carry_ref = refs[:2]
        refs = refs[2:]
        if first:
            sum_in_ref, refs = refs[0], refs[1:]
    out_ref, back_ref, s_ref = refs[0], refs[1], refs[-1]
    v, total = backward_body(sz, r_refs, zb_ref, t_ref, s_ref)
    cells = a_ref.shape[1]
    rows = slice(sz.start, sz.start + sz.rows)
    for q in range(sz.quads):
        lanes = slice(q * sz.width, (q + 1) * sz.width)
        part = v[q * sz.rows:(q + 1) * sz.rows]
        out = part * b_ref[:, lanes].astype(jnp.float32)
        back = part * a_ref[rows, lanes]
        if again:
            out = out + run_ref[:, lanes]
            back = back + carry_ref[:, lanes].astype(jnp.float32)
        out_ref[:, lanes] = out
        back_ref[:, lanes] = back.astype(back_ref.dtype)
    if first:
        sum_ref = refs[2]
        sum_ref[...] = total + sum_in_ref[...] if again else total
        if again:
            carried = carry_ref[:, cells:].astype(jnp.float32)
            total = total + jnp.sum(carried, axis=0, keepdims=True)
        tail = pieces(total)
        if sz.rows > tail.shape[0]:
            rest = jnp.zeros((sz.rows - tail.shape[0], LANES), jnp.float32)
            tail = jnp.concatenate([tail, rest], axis=0)
        back_ref[:, cells:] = tail.astype(back_ref.dtype)


def last_kernel(sz, plan, run_ref, sum_ref, *refs):
    got_refs, (out_ref, block_ref) = refs[:len(plan)], refs[len(plan):]
    cells = run_ref.shape[1]
    total = sum_ref[...]
    for cut, got_ref in zip(plan, got_refs):
        rows = slice(cut.start, cut.start + cut.rows)
        out_ref[rows] = run_ref[rows] + got_ref[:, :cells].astype(jnp.float32)
        if cut.start == 0:
            carried = got_ref[:, cells:].astype(jnp.float32)
            total = total + jnp.sum(carried, axis=0, keepdims=True)
    block_ref[...] = jnp.sum(total, axis=1, keepdims=True) / float(sz.length**3)


def call(kernel, outs, args, scratch=()):
    held = [pltpu.with_memory_space_constraint(arg, pltpu.VMEM) for arg in args]
    return pl.pallas_call(
        kernel,
        out_shape=[pltpu.VMEM(shape, kind) for shape, kind in outs],
        in_specs=[pl.BlockSpec(memory_space=pltpu.VMEM)] * len(args),
        out_specs=[pl.BlockSpec(memory_space=pltpu.VMEM)] * len(outs),
        scratch_shapes=list(scratch),
        compiler_params=pltpu.CompilerParams(vmem_limit_bytes=24 * 2**20),
    )(*held)


def after(value, before):
    return value if before is None else lax.optimization_barrier((value, before))[0]


def exchange(blocks):
    count = len(blocks)
    got = {0: blocks[0]}
    for k in range(count - 1, 0, -1):
        got[k] = lax.ppermute(blocks[k], "ga", [(d, d ^ k) for d in range(count)])
    return [got[k] for k in range(count)]


def chunk_rows(rows):
    least = 8
    return [rows - least, least] if rows > least else [rows]


def local(orbitals, retained):
    bands_dev, slab_rows, plane_cells = orbitals.shape
    assert bands_dev == 1
    length = retained.shape[0]
    groups = lax.axis_size("ga")
    sz = Sizes(length, slab_rows, groups, 0, slab_rows)
    plan, at = [], 0
    for rows in chunk_rows(slab_rows):
        plan.append(Sizes(length, slab_rows, groups, at, rows))
        at += rows
    z, zb, mine = tables([[sz], plan])
    lattice = orbitals.reshape(slab_rows, plane_cells)
    half, full = jnp.bfloat16, jnp.float32
    local_y = lax.axis_index("ga") * sz.cols + jnp.arange(sz.cols, dtype=jnp.int32)
    local_y = jnp.broadcast_to((wrapped(local_y, length) ** 2)[:, None, None], (sz.cols, 1, LANES))

    flat = (slab_rows, plane_cells)

    def lines(cut):
        return pltpu.VMEM((cut.pack, cut.quads * cut.rows, LANES), full)

    def mids(cut):
        return pltpu.VMEM((cut.pack, groups * cut.span, LANES), full)

    def forward(cut, visitors):
        there = [((cut.chunks, cut.span, LANES), half)] * groups
        kernel = partial(forward_kernel, cut)
        return call(kernel, there, [lattice, visitors, z, mine], [lines(cut)])

    def middle(cuts, which, got):
        outs = []
        for cut in cuts:
            tail = 16 if cut.start == 0 else 0
            outs += [((cut.chunks * cut.span + tail, LANES), half)] * groups
        scratch = [mids(cut) for cut in cuts] * 2
        kernel = partial(middle_kernel, cuts, which)
        sent = call(kernel, outs, got + [mine, screen], scratch)
        return [sent[c * groups:(c + 1) * groups] for c in range(len(cuts))]

    def crossed(cut, got, visitors, old):
        first = cut.start == 0
        outs = [
            ((cut.rows, plane_cells), full),
            ((cut.rows, plane_cells + (LANES if first else 0)), half),
        ]
        if first:
            outs.append(((1, LANES), full))
        kernel = partial(cross_kernel, cut, len(old) > 0)
        return call(kernel, outs, got + [lattice, visitors, zb, mine] + old, [lines(cut)])

    def pair(visitors, old, ahead=None):
        got, before = [], None
        for c, cut in enumerate(plan):
            before = forward(cut, after(visitors[c], before))
            got += exchange(before)
        got = after(got, ahead)
        sent = middle(plan, 1, got)
        fresh = [None] * len(plan)
        for c in reversed(range(len(plan))):
            fresh[c] = crossed(plan[c], exchange(sent[c]), visitors[c], old[c])
        return [part[0] for part in fresh], [part[1] for part in fresh], fresh[0][2]

    band_reach = max(1, lax.axis_size("band") // 8)
    visitors = []
    halves = call(
        partial(split_kernel, plan), [((cut.rows, plane_cells), half) for cut in plan], [lattice]
    )
    for chunk in halves:
        visitors.append(passed_along(chunk, "band", 1))
    screen = call(
        partial(screen_kernel, sz), [((sz.cols, length, LANES), full)], [retained, local_y]
    )[0]
    sent = forward(sz, lattice)
    visitors = [after(chunk, sent) for chunk in visitors]
    sent = middle([sz], 0, exchange(sent))[0]
    running, carried, total = pair(visitors, [[]] * len(plan), sent)

    def round_once(rounds_done, state):
        visitors, running, carried, total = state
        visitors = [passed_along(chunk, "band", 1) for chunk in visitors]
        carried = [passed_along(chunk, "band", 1) for chunk in carried]
        old = [list(both) for both in zip(running, carried)]
        old[0].append(total)
        running, carried, total = pair(visitors, old)
        return visitors, running, carried, total

    if band_reach > 1:
        state = (visitors, running, carried, total)
        visitors, running, carried, total = lax.fori_loop(1, band_reach, round_once, state)
    returned = []
    for chunk in carried:
        returned.append(passed_along(chunk, "band", -band_reach))
    running, total = call(
        partial(own_kernel, sz, plan),
        [(flat, full), ((1, LANES), full)],
        exchange(sent) + running + [lattice, total, zb, mine],
        [lines(sz)],
    )
    field, block = pl.pallas_call(
        partial(last_kernel, sz, plan),
        out_shape=[jax.ShapeDtypeStruct(flat, full), jax.ShapeDtypeStruct((1, 1), full)],
        compiler_params=pltpu.CompilerParams(vmem_limit_bytes=24 * 2**20),
        name="last",
    )(*[pltpu.with_memory_space_constraint(v, pltpu.VMEM) for v in [running, total] + returned])
    return field.reshape(orbitals.shape), block


def solution(mesh):
    placed = (P("band", "ga", None), P(None, "ga"))

    return jax.shard_map(
        local,
        mesh=mesh,
        in_specs=placed,
        out_specs=(P("band", "ga", None), P("band", None)),
        check_vma=False,
    )
```
